32 devices in a mesh: rep: 32 (over z, y, x, core).
Axes of the slice: x: 2, y: 2, z: 4, core: 2. Of those that a mesh axis runs over, the one named last changes fastest.
Arguments:
- inputs: bfloat16 [16384, 1024], P('rep'), may hold values from -6 to 6
- out_grads: bfloat16 [16384, 4096], P('rep'), may hold values from -0.29882812 to 0.29882812
- error_in: bfloat16 [32, 1024, 4096], P('rep'), may hold values from -6 to 6
- q_start: float32 [32, 4096], replicated, may hold values from -0.09375 to 0.09375
- master: float32 [1024, 4096], P(None, 'rep'), may hold values from -1.2 to 1.2
Outputs:
- error_out: bfloat16 [32, 1024, 4096], P('rep')
- q_out: float32 [32, 4096], replicated
- master_out: float32 [1024, 4096], P(None, 'rep')
The draws below stay inside these ranges and needn't reach their ends.
All inputs are finite; a program needn't handle non-finite values.
Results may differ from the reference program's by a relative error of at most 0.001.
Values sent between devices are 32-bit elements; how exact they have to be, the bound alone decides.
A program may use at most 128 MiB of HBM per device.

```python
import jax
import jax.numpy as jnp
from jax import lax

D = 1024
FF = 4096
RANK = 32
ITERS = 3
TOKENS = 16384
N_REP = 32


def steps_of(rng, shape, pieces, low, top_value):
    gain, own = 1.0, jax.random.fold_in(rng, 6)
    for position, parts in pieces:
        heights = jnp.exp(jax.random.uniform(jax.random.fold_in(own, position), (parts,), jnp.float32, low / len(pieces), top_value / len(pieces)))
        gain = gain * jnp.repeat(heights, shape[position] // parts).reshape([-1 if axis == position else 1 for axis in range(len(shape))])
    return gain


def gaussian(own_key, extent, spread, limit, pieces=(), held_as=jnp.bfloat16):
    result = jax.random.normal(own_key, extent, jnp.float32) * spread
    if len(pieces) > 0:
        result = steps_of(own_key, extent, pieces, -0.22, 0.18) * result
    return jnp.clip(result, min=-limit, max=limit).astype(held_as)


def setup_inputs(seed: int = 0) -> dict:
    splits = jax.random.split(jax.random.key(seed), 6)
    return {
        "inputs": gaussian(splits[0], (TOKENS, D), 1.0, 6.0, ((0, 32),)),
        "out_grads": gaussian(splits[1], (TOKENS, FF), 0.045, 0.29882812, ((0, 32),)),
        "error_in": gaussian(splits[2], (N_REP, D, FF), 1.0, 6.0, ((0, 32),)),
        "q_start": gaussian(splits[3], (RANK, FF), FF ** -0.5, 0.09375, (), jnp.float32),
        "master": gaussian(splits[4], (D, FF), 0.2, 1.2, ((1, 32),), jnp.float32),
    }


def orthonormal(rows):
    basis = jnp.zeros_like(rows)
    for k in range(rows.shape[0]):
        vector = rows[k]
        coef = jnp.dot(basis, vector, precision=lax.Precision.HIGHEST)
        vector = vector - jnp.dot(coef, basis, precision=lax.Precision.HIGHEST)
        basis = basis.at[k].set(vector / jnp.sqrt(jnp.sum(vector * vector) + 1.0))
    return basis

def reference(inputs, out_grads, error_in, q_start, master):
    tok = inputs.shape[0] // N_REP
    xs = inputs.reshape(N_REP, tok, inputs.shape[1])
    dys = out_grads.reshape(N_REP, tok, out_grads.shape[1])

    def one_replica(items):
        x_rows, dy_rows, error = items
        grad = lax.dot_general(x_rows, dy_rows, (((0,), (0,)), ((), ())), preferred_element_type=jnp.float32)
        return grad + error.astype(jnp.float32)
    merged = lax.map(one_replica, (xs, dys, error_in))
    merged_sum = lax.optimization_barrier(jnp.sum(merged, axis=0))
    factor = q_start
    basis = None
    for step in range(ITERS):
        p_total = lax.dot_general(factor, merged_sum, (((1,), (1,)), ((), ())), precision=lax.Precision.HIGHEST, preferred_element_type=jnp.float32)
        basis = orthonormal(p_total)
        factor = jnp.dot(basis, merged_sum, precision=lax.Precision.HIGHEST, preferred_element_type=jnp.float32) / N_REP
    recon = lax.dot_general(basis, factor, (((0,), (0,)), ((), ())), precision=lax.Precision.HIGHEST, preferred_element_type=jnp.float32)
    error_out = (merged - recon[None]).astype(jnp.bfloat16)
    master_out = master - 0.5 * recon
    return (error_out, factor, master_out)
```

```python
import functools

import jax
import jax.numpy as jnp
from jax import lax
from jax.experimental import pallas as pl
from jax.experimental.pallas import tpu as pltpu
from jax.sharding import PartitionSpec as P

ITERS = 3
AXIS = "rep"
CHUNK = 512
MESH = pl.DeviceIdType.MESH
F32, BF16 = jnp.float32, jnp.bfloat16


def split_tiles(count, rows, cols):
    col_cuts = min(count, cols // 128)
    row_cuts = max(1, min(count // col_cuts, rows // 8))
    return row_cuts, col_cuts, count // (row_cuts * col_cuts)


def split_columns(count, cols):
    col_cuts = min(count, cols // 128)
    return 1, col_cuts, count // col_cuts


def halves(value):
    high = value.astype(BF16)
    return high, (value - high.astype(F32)).astype(BF16)


def far_first(own, step, count):
    if count & (count - 1) == 0:
        return own ^ (count - step)
    return lax.rem(own + step, count)


def near_first(own, step, count):
    if count & (count - 1) == 0:
        return own ^ step
    return lax.rem(own - step + count, count)


def kernel(
    count, x_hbm, dy_hbm, err_hbm, start_hbm, master_hbm,
    err_out, q_out, master_out,
    x_v, xt_v, dy_v, merged, pair, m_hi, m_lo,
    q_full, q_part, q_recv, q_split, p_full, p_part, p_recv, vecs, basis, t_vecs, t_mat, b_split, b_tall, p_tall,
    load_sem, start_sem, master_sem, dy_sem, err_sem, pair_send, pair_recv, relay_send, relay_recv,
    p_rs_send, p_rs_recv, p_ag_send, p_ag_recv, q_rs_send, q_rs_recv, q_ag_send, q_ag_recv,
):
    me = lax.axis_index(AXIS)
    core, chip, chips = lax.rem(me, 2), me // 2, count // 2
    partner = me + 1 - 2 * core
    err_v = err_out.at[0]
    rank, width = p_full.shape
    ff = q_full.shape[1]
    half = ff // 2
    groups, _, cw = pair.shape
    own_base, other_base = core * half, (1 - core) * half

    def chunk(base, i):
        return pl.ds(pl.multiple_of(base + i * cw, cw), cw)

    def local(i):
        return pl.ds(pl.multiple_of(i * cw, cw), cw)

    own_half = pl.ds(pl.multiple_of(own_base, half), half)

    def chunk_loads(base, i, slot):
        cols = chunk(base, i)
        return (
            pltpu.make_async_copy(dy_hbm.at[:, cols], dy_v.at[:, cols], dy_sem.at[slot]),
            pltpu.make_async_copy(err_hbm.at[0, :, cols], err_v.at[:, cols], err_sem.at[slot]),
        )

    def start_loads(base, i, slot):
        for load in chunk_loads(base, i, slot):
            load.start()

    pltpu.make_async_copy(x_hbm, x_v, load_sem).start()
    start_loads(other_base, 0, 0)

    barrier = pltpu.get_barrier_semaphore()

    @pl.loop(1, count)
    def _(d):
        pl.semaphore_signal(barrier, inc=1, device_id=(lax.rem(me + d, count),), device_id_type=MESH)

    pltpu.make_async_copy(x_hbm, x_v, load_sem).wait()
    for i in range(1, groups):
        start_loads(other_base, i, i)
    for i in range(groups):
        start_loads(own_base, i, groups + i)
    start_load = pltpu.make_async_copy(start_hbm.at[:, own_half], q_full.at[:, own_half], start_sem)
    start_load.start()
    master_load = pltpu.make_async_copy(master_hbm, master_out, master_sem)
    master_load.start()
    xt_v[...] = x_v[...].T

    def piece(cuts, shape, owner):
        row_cuts, col_cuts, stride = cuts
        index = owner // stride
        rows, cols = shape[0] // row_cuts, shape[1] // col_cuts
        row = pl.multiple_of((index % row_cuts) * rows, rows)
        col = pl.multiple_of((index // row_cuts) * cols, cols)
        return row, rows, col, cols

    def window(cuts, shape, owner, shift=0):
        row, rows, col, cols = piece(cuts, shape, owner)
        return pl.ds(row, rows), pl.ds(pl.multiple_of(shift + col, cols), cols)

    def is_owner(cuts, place):
        return lax.rem(place, cuts[2]) == 0

    def guarded(cuts, place, body):
        if cuts[2] == 1:
            body()
        else:
            pl.when(is_owner(cuts, place))(body)

    def either(cuts, place, owner_body, other_body):
        if cuts[2] == 1:
            owner_body()
        else:
            pl.when(is_owner(cuts, place))(owner_body)
            pl.when(jnp.logical_not(is_owner(cuts, place)))(other_body)

    def drain(recv, sem, pieces):
        if pieces:
            ref = recv.at[pl.ds(0, pieces)]
            pltpu.make_async_copy(ref, ref, sem).wait()

    def drain_sends(cuts, place, peers, recv, rs_send, ag_send):
        owners = cuts[0] * cuts[1]

        def owner_body():
            drain(recv, rs_send, owners - 1)
            drain(recv, ag_send, peers - 1)

        either(cuts, place, owner_body, lambda: drain(recv, rs_send, owners))

    p_cuts = split_tiles(count, rank, width)
    q_cuts = split_columns(chips, half)
    p_owners, q_owners = p_cuts[0] * p_cuts[1], q_cuts[0] * q_cuts[1]
    members = cw // (half // q_cuts[1])
    own_group = chip // q_cuts[2] // members

    def absorb(group):
        high, low = halves(q_full[:, chunk(own_base, group)])
        factor = jnp.concatenate([high, low], axis=0)
        dims = (((1,), (1,)), ((), ()))
        cols = local(group)
        tall = lax.dot_general(m_hi[:, cols], factor, dims, preferred_element_type=F32)
        tall += lax.dot_general(m_lo[:, cols], factor, dims, preferred_element_type=F32)
        p_tall[...] += tall

    def settle():
        flat = p_tall[...].T
        p_part[...] = flat[0:rank] + flat[rank:2 * rank]

        @pl.loop(1, count)
        def _(d):
            target = far_first(me, d, count)

            def send():
                pltpu.make_async_remote_copy(
                    src_ref=p_part.at[window(p_cuts, p_part.shape, target)],
                    dst_ref=p_recv.at[lax.rem(target - me + count, count) - 1],
                    send_sem=p_rs_send, recv_sem=p_rs_recv,
                    device_id=(target,), device_id_type=MESH,
                ).start()

            guarded(p_cuts, target, send)

        p_tall[...] = jnp.zeros_like(p_tall)

    def merge(base, i, slot):
        cols = chunk(base, i)
        for load in chunk_loads(base, i, slot):
            load.wait()
        product = jnp.dot(xt_v[...], dy_v[:, cols], preferred_element_type=F32)
        merged[:, cols] = product + err_v[:, cols].astype(F32)
        return cols

    p_tall[...] = jnp.zeros_like(p_tall)
    pl.semaphore_wait(barrier, count - 1)

    @pl.loop(0, groups)
    def _(i):
        cols = merge(other_base, i, i)
        pltpu.make_async_remote_copy(
            src_ref=merged.at[:, cols], dst_ref=pair.at[i],
            send_sem=pair_send, recv_sem=pair_recv.at[i],
            device_id=(partner,), device_id_type=MESH,
        ).start()

    @pl.loop(0, groups)
    def _(i):
        merge(own_base, i, groups + i)

    start_load.wait()

    @pl.loop(0, groups)
    def _(i):
        pltpu.make_async_copy(pair.at[i], pair.at[i], pair_recv.at[i]).wait()
        high, low = halves(merged[:, chunk(own_base, i)] + pair[i])
        m_hi[:, local(i)] = high
        m_lo[:, local(i)] = low
        absorb(i)

    settle()
    pltpu.make_async_copy(pair, pair, pair_send).wait()

    def orthogonalize():
        vecs[...] = p_full[...]
        lanes = lax.broadcasted_iota(jnp.int32, t_vecs.shape, 1)
        t_vecs[...] = (lanes == lax.broadcasted_iota(jnp.int32, t_vecs.shape, 0)).astype(F32)
        for base in range(0, rank, 8):
            block = pl.ds(base, 8)
            above, rest, t_rest = p_full[block, :], vecs[block, :], t_vecs[block, :]
            done, t_done = [], []
            for k in range(8):
                row = rest[k:k + 1, :]
                norm = jnp.sum(row * row, axis=1, keepdims=True) + 1.0
                coef = jnp.sum(above * row, axis=1, keepdims=True)
                inverse = lax.rsqrt(norm)
                unit = row * inverse
                t_unit = t_rest[k:k + 1, :] * inverse
                done.append(unit)
                t_done.append(t_unit)
                if k < 7:
                    rest = rest - (coef * inverse) * unit
                    t_rest = t_rest - (coef * inverse) * t_unit
                for below in range(base + 8, rank, 8):
                    later = pl.ds(below, 8)
                    coef = jnp.sum(p_full[later, :] * unit, axis=1, keepdims=True)
                    vecs[later, :] = vecs[later, :] - coef * unit
                    t_vecs[later, :] = t_vecs[later, :] - coef * t_unit
            basis[block, :] = jnp.concatenate(done, axis=0)
            t_mat[block, :] = jnp.concatenate(t_done, axis=0)

    def sum_p():
        def body():
            mine = window(p_cuts, p_part.shape, me)
            drain(p_recv, p_rs_recv, count - 1)
            p_full[mine] = p_part[mine] + jnp.sum(p_recv[...], axis=0)

            @pl.loop(1, count)
            def _(d):
                pltpu.make_async_remote_copy(
                    src_ref=p_full.at[mine], dst_ref=p_full.at[mine],
                    send_sem=p_ag_send, recv_sem=p_ag_recv,
                    device_id=(far_first(me, d, count),), device_id_type=MESH,
                ).start()

        either(p_cuts, me, body, lambda: None)
        either(
            p_cuts, me,
            lambda: drain(p_recv, p_ag_recv, p_owners - 1),
            lambda: drain(p_recv, p_ag_recv, p_owners),
        )

    def sum_q():
        def body():
            drain(q_recv, q_rs_recv, chips - 1)
            total = q_part[window(q_cuts, q_part.shape, chip)] + jnp.sum(q_recv[...], axis=0)
            rotated = jnp.dot(
                t_mat[:, 0:rank], total, precision=lax.Precision.HIGHEST, preferred_element_type=F32
            )
            mine = window(q_cuts, q_part.shape, chip, own_base)
            q_full[mine] = rotated / count

            @pl.loop(1, chips)
            def _(d):
                pltpu.make_async_remote_copy(
                    src_ref=q_full.at[mine], dst_ref=q_full.at[mine],
                    send_sem=q_ag_send, recv_sem=q_ag_recv.at[own_group],
                    device_id=(2 * far_first(chip, d, chips) + core,), device_id_type=MESH,
                ).start()

        either(q_cuts, chip, body, lambda: None)

    def await_group(group):
        def own_or_other():
            @pl.when(group == own_group)
            def _():
                drain(q_recv, q_ag_recv.at[group], members - 1)

            @pl.when(group != own_group)
            def _():
                drain(q_recv, q_ag_recv.at[group], members)

        either(q_cuts, chip, own_or_other, lambda: drain(q_recv, q_ag_recv.at[group], members))

    @pl.loop(0, ITERS)
    def _(step):
        sum_p()
        high, low = halves(p_full[...])
        b_split[0:rank] = high
        b_split[rank:2 * rank] = low

        @pl.loop(0, groups)
        def _(i):
            group = far_first(own_group, i + 1, groups)
            cols = local(group)
            both = jnp.dot(b_split[...], m_hi[:, cols], preferred_element_type=F32)
            both += jnp.dot(b_split[...], m_lo[:, cols], preferred_element_type=F32)
            q_part[:, cols] = both[0:rank] + both[rank:2 * rank]

            for j in range(members):
                target = (group * members + j) * q_cuts[2]

                @pl.when(target != chip)
                def _():
                    pltpu.make_async_remote_copy(
                        src_ref=q_part.at[window(q_cuts, q_part.shape, target)],
                        dst_ref=q_recv.at[lax.rem(target - chip + chips, chips) - 1],
                        send_sem=q_rs_send, recv_sem=q_rs_recv,
                        device_id=(2 * target + core,), device_id_type=MESH,
                    ).start()

        orthogonalize()
        sum_q()
        drain_sends(p_cuts, me, count, p_recv, p_rs_send, p_ag_send)

        @pl.when(step < ITERS - 1)
        def _():
            @pl.loop(0, groups)
            def _(i):
                group = near_first(own_group, i, groups)
                await_group(group)
                absorb(group)

            settle()
            drain_sends(q_cuts, chip, chips, q_recv, q_rs_send, q_ag_send)

    tall = basis[...].T
    high, low = halves(tall)
    b_tall[:, 0:rank] = high
    b_tall[:, rank:2 * rank] = high
    b_tall[:, 2 * rank:3 * rank] = low

    def finish(cols):
        high, low = halves(q_full[:, cols])
        factor = jnp.concatenate([high, low, high], axis=0)
        q_split[:, cols] = factor
        recon = jnp.dot(b_tall[...], factor, preferred_element_type=F32)
        err_v[:, cols] = (merged[:, cols] - recon).astype(BF16)

    def relay(base, group):
        cols = chunk(base, group)
        return pltpu.make_async_remote_copy(
            src_ref=q_full.at[:, cols], dst_ref=q_full.at[:, cols],
            send_sem=relay_send, recv_sem=relay_recv.at[group],
            device_id=(partner,), device_id_type=MESH,
        )

    @pl.loop(0, groups)
    def _(i):
        group = near_first(own_group, i, groups)
        await_group(group)
        relay(own_base, group).start()
        finish(chunk(own_base, group))

    @pl.loop(0, groups)
    def _(i):
        group = near_first(own_group, i, groups)
        relay(other_base, group).wait_recv()
        finish(chunk(other_base, group))

    drain_sends(q_cuts, chip, chips, q_recv, q_rs_send, q_ag_send)
    pltpu.make_async_copy(q_part, q_part, relay_send).wait()
    q_out[...] = q_full[...]

    own = master_out.shape[1]
    if own % 128 == 0:
        mine = q_split[:, pl.ds(pl.multiple_of(me * own, own), own)]
    else:
        base = pl.multiple_of((me * own) // 128 * 128, 128)
        block = q_split[:, pl.ds(base, 128)].astype(F32)
        shift = lax.rem(128 - lax.rem(me * own, 128), 128)
        mine = pltpu.roll(block, shift, 1)[:, 0:own].astype(BF16)
    master_load.wait()
    master_out[...] = master_out[...] - 0.5 * jnp.dot(b_tall[...], mine, preferred_element_type=F32)


def shards(inputs, out_grads, error_in, q_start, master):
    count = lax.axis_size(AXIS)
    tokens, width = inputs.shape
    ff = out_grads.shape[1]
    rank = q_start.shape[0]
    chips, half = count // 2, ff // 2
    groups = half // CHUNK
    hbm_spec = pl.BlockSpec(memory_space=pltpu.HBM)
    vmem_spec = pl.BlockSpec(memory_space=pltpu.VMEM)
    p_cuts, q_cuts = split_tiles(count, rank, width), split_columns(chips, half)
    dma = pltpu.SemaphoreType.DMA
    return pl.pallas_call(
        functools.partial(kernel, count),
        out_shape=(
            pltpu.VMEM(error_in.shape, BF16),
            pltpu.VMEM(q_start.shape, F32),
            pltpu.VMEM(master.shape, F32),
        ),
        in_specs=[hbm_spec] * 5,
        out_specs=(vmem_spec, vmem_spec, vmem_spec),
        scratch_shapes=[
            pltpu.VMEM((tokens, width), BF16),
            pltpu.VMEM((width, tokens), BF16),
            pltpu.VMEM((tokens, ff), BF16),
            pltpu.VMEM((width, ff), F32),
            pltpu.VMEM((groups, width, CHUNK), F32),
            pltpu.VMEM((width, half), BF16),
            pltpu.VMEM((width, half), BF16),
            pltpu.VMEM((rank, ff), F32),
            pltpu.VMEM((rank, half), F32),
            pltpu.VMEM((chips - 1, rank // q_cuts[0], half // q_cuts[1]), F32),
            pltpu.VMEM((3 * rank, ff), BF16),
            pltpu.VMEM((rank, width), F32),
            pltpu.VMEM((rank, width), F32),
            pltpu.VMEM((count - 1, rank // p_cuts[0], width // p_cuts[1]), F32),
            pltpu.VMEM((rank, width), F32),
            pltpu.VMEM((rank, width), F32),
            pltpu.VMEM((rank, 128), F32),
            pltpu.VMEM((rank, 128), F32),
            pltpu.VMEM((2 * rank, width), BF16),
            pltpu.VMEM((width, 3 * rank), BF16),
            pltpu.VMEM((width, 2 * rank), F32),
            dma, dma, dma, dma((2 * groups,)), dma((2 * groups,)), dma, dma((groups,)), dma, dma((groups,)),
            dma, dma, dma, dma, dma, dma, dma, dma((groups,)),
        ],
        compiler_params=pltpu.CompilerParams(
            collective_id=0, has_side_effects=True, vmem_limit_bytes=52 * 1024 * 1024
        ),
    )(inputs, out_grads, error_in, q_start, master)


def solution(mesh):
    return jax.shard_map(
        shards,
        mesh=mesh,
        in_specs=(P("rep", None), P("rep", None), P("rep", None, None), P(), P(None, "rep")),
        out_specs=(P("rep", None, None), P(), P(None, "rep")),
        check_vma=False,
    )
```

```python
import functools

import jax
import jax.numpy as jnp
from jax import lax
from jax.experimental import pallas as pl
from jax.experimental.pallas import tpu as pltpu
from jax.sharding import PartitionSpec as P

ITERS = 3
AXIS = "rep"
CHUNK = 512
EARLY, LATE = 2, 3
MESH = pl.DeviceIdType.MESH
F32, BF16 = jnp.float32, jnp.bfloat16


def split_tiles(count, rows, cols):
    col_cuts = min(count, cols // 128)
    row_cuts = max(1, min(count // col_cuts, rows // 8))
    return row_cuts, col_cuts, count // (row_cuts * col_cuts)


def split_columns(count, cols):
    col_cuts = min(count, cols // 128)
    return 1, col_cuts, count // col_cuts


def halves(value):
    high = value.astype(BF16)
    return high, (value - high.astype(F32)).astype(BF16)


def far_first(own, step, count):
    if count & (count - 1) == 0:
        return own ^ (count - step)
    return lax.rem(own + step, count)


def near_first(own, step, count):
    if count & (count - 1) == 0:
        return own ^ step
    return lax.rem(own - step + count, count)


def kernel(
    count, x_hbm, dy_hbm, err_hbm, start_hbm,
    err_own, rest, q_out, b_tall,
    x_v, xt_v, dy_v, err_v, merged, pair, m_hi, m_lo,
    q_full, q_part, q_recv, b_split, p_full, p_part, p_recv, vecs, basis, t_vecs, t_mat, p_tall, u_tall, p_flat,
    load_sem, start_sem, dy_sem, err_sem, pair_send, pair_recv, relay_send, relay_recv,
    p_rs_send, p_rs_recv, p_ag_send, p_ag_recv, q_rs_send, q_rs_recv, q_ag_send, q_ag_recv,
):
    me = lax.axis_index(AXIS)
    core, chip, chips = lax.rem(me, 2), me // 2, count // 2
    partner = me + 1 - 2 * core
    rank, width = p_full.shape
    ff = q_full.shape[1]
    half = ff // 2
    groups, _, cw = pair.shape
    own_base, other_base = core * half, (1 - core) * half

    def chunk(base, i):
        return pl.ds(pl.multiple_of(base + i * cw, cw), cw)

    def local(i):
        return pl.ds(pl.multiple_of(i * cw, cw), cw)

    def chunk_loads(base, i, slot):
        cols = chunk(base, i)
        return (
            pltpu.make_async_copy(dy_hbm.at[:, cols], dy_v.at[:, cols], dy_sem.at[slot]),
            pltpu.make_async_copy(err_hbm.at[0, :, cols], err_v.at[:, cols], err_sem.at[slot]),
        )

    def start_loads(base, i, slot):
        for load in chunk_loads(base, i, slot):
            load.start()

    pltpu.make_async_copy(x_hbm, x_v, load_sem).start()
    start_load = pltpu.make_async_copy(start_hbm, q_full, start_sem)
    start_load.start()
    start_loads(other_base, 0, 0)

    barrier = pltpu.get_barrier_semaphore()

    @pl.loop(1, count)
    def _(d):
        pl.semaphore_signal(barrier, inc=1, device_id=(lax.rem(me + d, count),), device_id_type=MESH)

    pltpu.make_async_copy(x_hbm, x_v, load_sem).wait()
    for i in range(1, groups):
        start_loads(other_base, i, i)
    for i in range(groups):
        start_loads(own_base, i, groups + i)
    xt_v[...] = x_v[...].T

    def owner_of(cuts, index):
        return index * cuts[2]

    def index_of(cuts, place):
        return place // cuts[2]

    def window(cuts, shape, index, shift=0):
        row_cuts, col_cuts = cuts[:2]
        rows, cols = shape[0] // row_cuts, shape[1] // col_cuts
        row = pl.multiple_of(lax.rem(index, row_cuts) * rows, rows)
        col = pl.multiple_of(shift + index // row_cuts * cols, cols)
        return pl.ds(row, rows), pl.ds(col, cols)

    def either(cuts, place, owner_body, other_body):
        if cuts[2] == 1:
            owner_body()
        else:
            owns = jnp.logical_and(lax.rem(place, cuts[2]) == 0, place < cuts[0] * cuts[1] * cuts[2])
            pl.when(owns)(owner_body)
            pl.when(jnp.logical_not(owns))(other_body)

    def drain(recv, sem, pieces):
        if pieces:
            ref = recv.at[pl.ds(0, pieces)]
            pltpu.make_async_copy(ref, ref, sem).wait()

    def drain_sends(cuts, place, peers, recv, rs_send, ag_send):
        owners = cuts[0] * cuts[1]

        def owner_body():
            drain(recv, rs_send, owners - 1)
            drain(recv, ag_send, peers - 1)

        either(cuts, place, owner_body, lambda: drain(recv, rs_send, owners))

    p_cuts = split_tiles(count, rank, width)
    q_cuts = split_columns(chips, half)
    p_owners, q_owners = p_cuts[0] * p_cuts[1], q_cuts[0] * q_cuts[1]
    members = cw // (half // q_cuts[1])
    own_group = jnp.minimum(index_of(q_cuts, chip), q_owners - 1) // members

    def split_factor(cols):
        high, low = halves(q_full[:, cols])
        return jnp.concatenate([high, low], axis=0)

    def tall_dot(left, factor):
        return lax.dot_general(left, factor, (((1,), (1,)), ((), ())), preferred_element_type=F32)

    block = max(256, width // p_cuts[1])
    blocks = width // block
    sharers = p_cuts[0] * (block // (width // p_cuts[1]))
    own_block = jnp.minimum(index_of(p_cuts, me), p_owners - 1) // sharers

    def block_of(index):
        return pl.ds(pl.multiple_of(index * block, block), block)

    def send_block(index):
        for j in range(sharers):
            place = index * sharers + j
            target = owner_of(p_cuts, place)

            @pl.when(target != me)
            def _():
                pltpu.make_async_remote_copy(
                    src_ref=p_part.at[window(p_cuts, p_part.shape, place)],
                    dst_ref=p_recv.at[lax.rem(target - me + count, count) - 1],
                    send_sem=p_rs_send, recv_sem=p_rs_recv,
                    device_id=(target,), device_id_type=MESH,
                ).start()

    def absorb(group):
        factor = split_factor(chunk(own_base, group))
        cols = local(group)
        p_flat[...] += tall_dot(factor, m_hi[:, cols]) + tall_dot(factor, m_lo[:, cols])

    def absorb_last(group):
        factor = split_factor(chunk(own_base, group))
        cols = local(group)

        @pl.loop(0, blocks)
        def _(i):
            index = far_first(own_block, i + 1, blocks)
            rows = block_of(index)
            flat = p_flat[:, rows] + tall_dot(factor, m_hi[rows, cols]) + tall_dot(factor, m_lo[rows, cols])
            p_part[:, rows] = flat[0:rank] + flat[rank:2 * rank]
            send_block(index)

        p_flat[...] = jnp.zeros_like(p_flat)

    def merge(base, i, into):
        cols = chunk(base, i)
        product = jnp.dot(xt_v[...], dy_v[:, cols], preferred_element_type=F32)
        into[:, local(i)] = product + err_v[:, cols].astype(F32)

    def await_loads(base, i, slot):
        for load in chunk_loads(base, i, slot):
            load.wait()

    def first_factor(base, i):
        cols = chunk(base, i)
        factor = split_factor(cols)
        p_tall[...] += tall_dot(err_v[:, cols], factor)
        u_tall[...] += tall_dot(dy_v[:, cols], factor)

    def send_pair(i):
        pltpu.make_async_remote_copy(
            src_ref=rest.at[:, local(i)], dst_ref=pair.at[i],
            send_sem=pair_send, recv_sem=pair_recv.at[i],
            device_id=(partner,), device_id_type=MESH,
        ).start()

    p_tall[...] = jnp.zeros_like(p_tall)
    u_tall[...] = jnp.zeros_like(u_tall)
    pl.semaphore_wait(barrier, count - 1)
    start_load.wait()

    @pl.loop(0, groups)
    def _(i):
        await_loads(other_base, i, i)
        first_factor(other_base, i)

        @pl.when(i < EARLY)
        def _():
            merge(other_base, i, rest)
            send_pair(i)

    @pl.loop(0, groups)
    def _(i):
        await_loads(own_base, i, groups + i)
        first_factor(own_base, i)

    u_flat = u_tall[...].T
    high, low = halves(u_flat[0:rank] + u_flat[rank:2 * rank])
    u_split = jnp.concatenate([high, low], axis=0)

    @pl.loop(0, blocks)
    def _(i):
        index = far_first(own_block, i + 1, blocks)
        cols = block_of(index)
        flat = p_tall[cols, :].T + jnp.dot(u_split, x_v[:, cols], preferred_element_type=F32)
        p_part[:, cols] = flat[0:rank] + flat[rank:2 * rank]
        send_block(index)

    p_flat[...] = jnp.zeros_like(p_flat)

    @pl.loop(EARLY, groups)
    def _(i):
        merge(other_base, i, rest)
        pl.when(i < LATE)(lambda: send_pair(i))

    @pl.loop(0, groups // 2)
    def _(i):
        merge(own_base, i, merged)

    def add_pair():
        for i in range(LATE, groups):
            send_pair(i)

        @pl.loop(groups // 2, groups)
        def _(i):
            merge(own_base, i, merged)

        @pl.loop(0, groups)
        def _(i):
            pltpu.make_async_copy(pair.at[i], pair.at[i], pair_recv.at[i]).wait()
            high, low = halves(merged[:, local(i)] + pair[i])
            m_hi[:, local(i)] = high
            m_lo[:, local(i)] = low

        pltpu.make_async_copy(pair, pair, pair_send).wait()

    def orthogonalize():
        vecs[...] = p_full[...]
        lanes = lax.broadcasted_iota(jnp.int32, t_vecs.shape, 1)
        t_vecs[...] = (lanes == lax.broadcasted_iota(jnp.int32, t_vecs.shape, 0)).astype(F32)
        for base in range(0, rank, 8):
            band = pl.ds(base, 8)
            above, left, t_left = p_full[band, :], vecs[band, :], t_vecs[band, :]
            done, t_done = [], []
            for k in range(8):
                row = left[k:k + 1, :]
                norm = jnp.sum(row * row, axis=1, keepdims=True) + 1.0
                coef = jnp.sum(above * row, axis=1, keepdims=True)
                inverse = lax.rsqrt(norm)
                unit = row * inverse
                t_unit = t_left[k:k + 1, :] * inverse
                done.append(unit)
                t_done.append(t_unit)
                if k < 7:
                    left = left - (coef * inverse) * unit
                    t_left = t_left - (coef * inverse) * t_unit
                for below in range(base + 8, rank, 8):
                    later = pl.ds(below, 8)
                    coef = jnp.sum(p_full[later, :] * unit, axis=1, keepdims=True)
                    vecs[later, :] = vecs[later, :] - coef * unit
                    t_vecs[later, :] = t_vecs[later, :] - coef * t_unit
            basis[band, :] = jnp.concatenate(done, axis=0)
            t_mat[band, :] = jnp.concatenate(t_done, axis=0)

    def sum_p():
        def body():
            mine = window(p_cuts, p_part.shape, index_of(p_cuts, me))
            drain(p_recv, p_rs_recv, count - 1)
            p_full[mine] = p_part[mine] + jnp.sum(p_recv[...], axis=0)

            @pl.loop(1, count)
            def _(d):
                pltpu.make_async_remote_copy(
                    src_ref=p_full.at[mine], dst_ref=p_full.at[mine],
                    send_sem=p_ag_send, recv_sem=p_ag_recv.at[own_block],
                    device_id=(far_first(me, d, count),), device_id_type=MESH,
                ).start()

        either(p_cuts, me, body, lambda: None)

    def await_block(index):
        def own_or_other():
            @pl.when(index == own_block)
            def _():
                drain(p_recv, p_ag_recv.at[index], sharers - 1)

            @pl.when(index != own_block)
            def _():
                drain(p_recv, p_ag_recv.at[index], sharers)

        either(p_cuts, me, own_or_other, lambda: drain(p_recv, p_ag_recv.at[index], sharers))

    def send_group(group):
        for j in range(members):
            place = group * members + j
            target = owner_of(q_cuts, place)

            @pl.when(target != chip)
            def _():
                pltpu.make_async_remote_copy(
                    src_ref=q_part.at[window(q_cuts, q_part.shape, place)],
                    dst_ref=q_recv.at[lax.rem(target - chip + chips, chips) - 1],
                    send_sem=q_rs_send, recv_sem=q_rs_recv,
                    device_id=(2 * target + core,), device_id_type=MESH,
                ).start()

    def multiply():
        @pl.loop(0, blocks)
        def _(i):
            await_block(near_first(own_block, i, blocks))

        high, low = halves(p_full[...])
        left = jnp.concatenate([high, low], axis=0)
        b_split[...] = left

        @pl.loop(0, groups)
        def _(i):
            group = far_first(own_group, i + 1, groups)
            cols = local(group)
            both = jnp.dot(b_split[...], m_hi[:, cols], preferred_element_type=F32)
            both += jnp.dot(b_split[...], m_lo[:, cols], preferred_element_type=F32)
            q_part[:, cols] = both[0:rank] + both[rank:2 * rank]
            send_group(group)

    def sum_q():
        def body():
            drain(q_recv, q_rs_recv, chips - 1)
            index = index_of(q_cuts, chip)
            total = q_part[window(q_cuts, q_part.shape, index)] + jnp.sum(q_recv[...], axis=0)
            rotated = jnp.dot(
                t_mat[:, 0:rank], total, precision=lax.Precision.HIGHEST, preferred_element_type=F32
            )
            mine = window(q_cuts, q_part.shape, index, own_base)
            q_full[mine] = rotated / count

            @pl.loop(1, chips)
            def _(d):
                pltpu.make_async_remote_copy(
                    src_ref=q_full.at[mine], dst_ref=q_full.at[mine],
                    send_sem=q_ag_send, recv_sem=q_ag_recv.at[own_group],
                    device_id=(2 * far_first(chip, d, chips) + core,), device_id_type=MESH,
                ).start()

        either(q_cuts, chip, body, lambda: None)

    def await_group(group):
        def own_or_other():
            @pl.when(group == own_group)
            def _():
                drain(q_recv, q_ag_recv.at[group], members - 1)

            @pl.when(group != own_group)
            def _():
                drain(q_recv, q_ag_recv.at[group], members)

        either(q_cuts, chip, own_or_other, lambda: drain(q_recv, q_ag_recv.at[group], members))

    @pl.loop(0, ITERS)
    def _(step):
        sum_p()
        pl.when(step == 0)(add_pair)
        multiply()
        orthogonalize()
        sum_q()
        drain_sends(p_cuts, me, count, p_recv, p_rs_send, p_ag_send)

        @pl.when(step < ITERS - 1)
        def _():
            @pl.loop(0, groups - 1)
            def _(i):
                group = near_first(own_group, i, groups)
                await_group(group)
                absorb(group)

            group = near_first(own_group, groups - 1, groups)
            await_group(group)
            absorb_last(group)
            drain_sends(q_cuts, chip, chips, q_recv, q_rs_send, q_ag_send)

    tall = basis[...].T
    high, low = halves(tall)
    b_tall[:, 0:rank] = high
    b_tall[:, rank:2 * rank] = high
    b_tall[:, 2 * rank:3 * rank] = low

    def relay(base, group):
        cols = chunk(base, group)
        return pltpu.make_async_remote_copy(
            src_ref=q_full.at[:, cols], dst_ref=q_full.at[:, cols],
            send_sem=relay_send, recv_sem=relay_recv.at[group],
            device_id=(partner,), device_id_type=MESH,
        )

    @pl.loop(0, groups)
    def _(i):
        group = near_first(own_group, i, groups)
        await_group(group)
        relay(own_base, group).start()
        cols = local(group)
        err_own[:, cols] = (merged[:, cols] - recon(b_tall, q_full, chunk(own_base, group))).astype(BF16)

    @pl.loop(0, groups)
    def _(i):
        relay(other_base, i).wait_recv()

    drain_sends(q_cuts, chip, chips, q_recv, q_rs_send, q_ag_send)
    pltpu.make_async_copy(q_part, q_part, relay_send).wait()
    q_out[...] = q_full[...]


def recon(b_tall, q_full, cols):
    high, low = halves(q_full[:, cols])
    factor = jnp.concatenate([high, low, high], axis=0)
    return jnp.dot(b_tall[...], factor, preferred_element_type=F32)


def finish(
    err_own, rest, q_full, b_tall, master_hbm, err_out, q_out, master_out, tiles, master_v, load_sem, send_sem
):
    me = lax.axis_index(AXIS)
    core = lax.rem(me, 2)
    groups, _, cw = tiles.shape
    half = groups * cw
    own_base, other_base = core * half, (1 - core) * half
    load = pltpu.make_async_copy(master_hbm, master_v, load_sem)
    load.start()
    own_store = pltpu.make_async_copy(
        err_own, err_out.at[0, :, pl.ds(pl.multiple_of(own_base, half), half)], send_sem.at[groups]
    )
    own_store.start()
    q_store = pltpu.make_async_copy(q_full, q_out, send_sem.at[groups + 1])
    q_store.start()

    def store(i):
        cols = pl.ds(pl.multiple_of(other_base + i * cw, cw), cw)
        return pltpu.make_async_copy(tiles.at[i], err_out.at[0, :, cols], send_sem.at[i])

    @pl.loop(0, groups)
    def _(i):
        cols = pl.ds(pl.multiple_of(other_base + i * cw, cw), cw)
        local = pl.ds(pl.multiple_of(i * cw, cw), cw)
        tiles[i] = (rest[:, local] - recon(b_tall, q_full, cols)).astype(BF16)
        store(i).start()

    own = master_v.shape[1]
    span = max(own, 128)
    base = pl.multiple_of((me * own) // span * span, span)
    change = recon(b_tall, q_full, pl.ds(base, span))
    if own < span:
        change = pltpu.roll(change, lax.rem(span - lax.rem(me * own, span), span), 1)[:, 0:own]
    load.wait()
    master_v[...] = master_v[...] - 0.5 * change
    master_store = pltpu.make_async_copy(master_v, master_out, send_sem.at[groups + 2])
    master_store.start()

    @pl.loop(0, groups)
    def _(i):
        store(i).wait()

    own_store.wait()
    q_store.wait()
    master_store.wait()


def shards(inputs, out_grads, error_in, q_start, master):
    count = lax.axis_size(AXIS)
    tokens, width = inputs.shape
    ff = out_grads.shape[1]
    rank = q_start.shape[0]
    chips, half = count // 2, ff // 2
    groups = half // CHUNK
    hbm_spec = pl.BlockSpec(memory_space=pltpu.HBM)
    vmem_spec = pl.BlockSpec(memory_space=pltpu.VMEM)
    p_cuts, q_cuts = split_tiles(count, rank, width), split_columns(chips, half)
    blocks = width // max(256, width // p_cuts[1])
    dma = pltpu.SemaphoreType.DMA
    parts = pl.pallas_call(
        functools.partial(kernel, count),
        out_shape=(
            pltpu.VMEM((width, half), BF16),
            pltpu.VMEM((width, half), F32),
            pltpu.VMEM((rank, ff), F32),
            pltpu.VMEM((width, 3 * rank), BF16),
        ),
        in_specs=[hbm_spec] * 4,
        out_specs=(vmem_spec,) * 4,
        scratch_shapes=[
            pltpu.VMEM((tokens, width), BF16),
            pltpu.VMEM((width, tokens), BF16),
            pltpu.VMEM((tokens, ff), BF16),
            pltpu.VMEM((width, ff), BF16),
            pltpu.VMEM((width, half), F32),
            pltpu.VMEM((groups, width, CHUNK), F32),
            pltpu.VMEM((width, half), BF16),
            pltpu.VMEM((width, half), BF16),
            pltpu.VMEM((rank, ff), F32),
            pltpu.VMEM((rank, half), F32),
            pltpu.VMEM((chips - 1, rank // q_cuts[0], half // q_cuts[1]), F32),
            pltpu.VMEM((2 * rank, width), BF16),
            pltpu.VMEM((rank, width), F32),
            pltpu.VMEM((rank, width), F32),
            pltpu.VMEM((count - 1, rank // p_cuts[0], width // p_cuts[1]), F32),
            pltpu.VMEM((rank, width), F32),
            pltpu.VMEM((rank, width), F32),
            pltpu.VMEM((rank, 128), F32),
            pltpu.VMEM((rank, 128), F32),
            pltpu.VMEM((width, 2 * rank), F32),
            pltpu.VMEM((tokens, 2 * rank), F32),
            pltpu.VMEM((2 * rank, width), F32),
            dma, dma, dma((2 * groups,)), dma((2 * groups,)), dma, dma((groups,)), dma, dma((groups,)),
            dma, dma, dma, dma((blocks,)), dma, dma, dma, dma((groups,)),
        ],
        compiler_params=pltpu.CompilerParams(
            collective_id=0, has_side_effects=True, vmem_limit_bytes=47 * 1024 * 1024
        ),
    )(inputs, out_grads, error_in, q_start)
    return pl.pallas_call(
        finish,
        out_shape=(
            jax.ShapeDtypeStruct(error_in.shape, BF16),
            jax.ShapeDtypeStruct(q_start.shape, F32),
            jax.ShapeDtypeStruct(master.shape, F32),
        ),
        in_specs=[vmem_spec] * 4 + [hbm_spec],
        out_specs=(hbm_spec,) * 3,
        scratch_shapes=[
            pltpu.VMEM((groups, width, CHUNK), BF16),
            pltpu.VMEM(master.shape, F32),
            dma, dma((groups + 3,)),
        ],
        compiler_params=pltpu.CompilerParams(vmem_limit_bytes=16 * 1024 * 1024),
    )(*parts, master)


def solution(mesh):
    return jax.shard_map(
        shards,
        mesh=mesh,
        in_specs=(P("rep", None), P("rep", None), P("rep", None, None), P(), P(None, "rep")),
        out_specs=(P("rep", None, None), P(), P(None, "rep")),
        check_vma=False,
    )
```

```python
import functools

import jax
import jax.numpy as jnp
from jax import lax
from jax.experimental import pallas as pl
from jax.experimental.pallas import tpu as pltpu
from jax.sharding import PartitionSpec as P

ITERS = 3
STREAMS = 2
MIDDLE = True
AXIS = "rep"
CHUNK = 512
EARLY, LATE = 2, 3
MESH = pl.DeviceIdType.MESH
F32, BF16 = jnp.float32, jnp.bfloat16


def split_tiles(count, rows, cols):
    pool, first = (count // 2, count // 4) if MIDDLE and count % 4 == 0 else (count, 0)
    col_cuts = min(pool, cols // 128)
    row_cuts = max(1, min(pool // col_cuts, rows // 8))
    return row_cuts, col_cuts, pool // (row_cuts * col_cuts), first


def split_columns(count, cols):
    col_cuts = min(count, cols // 128)
    return 1, col_cuts, count // col_cuts, 0


def halves(value):
    high = value.astype(BF16)
    return high, (value - high.astype(F32)).astype(BF16)


def far_first(own, step, count):
    if count & (count - 1) == 0:
        return own ^ (count - step)
    return lax.rem(own + step, count)


def near_first(own, step, count):
    if count & (count - 1) == 0:
        return own ^ step
    return lax.rem(own - step + count, count)


def kernel(
    count, x_hbm, dy_hbm, err_hbm, start_hbm,
    err_own, rest, q_out, b_tall,
    x_v, xt_v, dy_v, err_v, merged, pair, m_hi, m_lo,
    q_full, q_part, q_recv, q_sum, p_full, p_part, p_recv, vecs, basis, t_vecs, t_mat, p_tall, u_tall, p_flat,
    load_sem, start_sem, dy_sem, err_sem, pair_send, pair_recv, relay_send, relay_recv,
    p_rs_send, p_rs_recv, p_ag_send, p_ag_recv, q_rs_send, q_rs_recv, q_ag_send, q_ag_recv,
):
    me = lax.axis_index(AXIS)
    core, chip, chips = lax.rem(me, 2), me // 2, count // 2
    partner = me + 1 - 2 * core
    rank, width = p_full.shape
    band = rank // STREAMS
    ff = q_full.shape[1]
    half = ff // 2
    groups, _, cw = pair.shape
    own_base, other_base = core * half, (1 - core) * half

    def chunk(base, i):
        return pl.ds(pl.multiple_of(base + i * cw, cw), cw)

    def local(i):
        return pl.ds(pl.multiple_of(i * cw, cw), cw)

    def chunk_loads(base, i, slot):
        cols = chunk(base, i)
        return (
            pltpu.make_async_copy(dy_hbm.at[:, cols], dy_v.at[:, cols], dy_sem.at[slot]),
            pltpu.make_async_copy(err_hbm.at[0, :, cols], err_v.at[:, cols], err_sem.at[slot]),
        )

    def start_loads(base, i, slot):
        for load in chunk_loads(base, i, slot):
            load.start()

    pltpu.make_async_copy(x_hbm, x_v, load_sem).start()
    start_load = pltpu.make_async_copy(start_hbm, q_full, start_sem)
    start_load.start()
    start_loads(other_base, 0, 0)

    barrier = pltpu.get_barrier_semaphore()

    @pl.loop(1, count)
    def _(d):
        pl.semaphore_signal(barrier, inc=1, device_id=(lax.rem(me + d, count),), device_id_type=MESH)

    pltpu.make_async_copy(x_hbm, x_v, load_sem).wait()
    for i in range(1, groups):
        start_loads(other_base, i, i)
    for i in range(groups):
        start_loads(own_base, i, groups + i)
    xt_v[...] = x_v[...].T

    def rows_of(h):
        return pl.ds(h * band, band)

    def owner_of(cuts, index):
        return cuts[3] + index * cuts[2]

    def index_of(cuts, place):
        return jnp.clip((place - cuts[3]) // cuts[2], 0, cuts[0] * cuts[1] - 1)

    def window(cuts, cols, index, h, shift=0):
        row_cuts, col_cuts = cuts[:2]
        rows, cols = band // row_cuts, cols // col_cuts
        row = pl.multiple_of(h * band + lax.rem(index, row_cuts) * rows, rows)
        col = pl.multiple_of(shift + index // row_cuts * cols, cols)
        return pl.ds(row, rows), pl.ds(col, cols)

    def either(cuts, place, peers, owner_body, other_body):
        row_cuts, col_cuts, stride, first = cuts
        if row_cuts * col_cuts == peers:
            owner_body()
        else:
            inside = jnp.logical_and(place >= first, place < first + row_cuts * col_cuts * stride)
            owns = jnp.logical_and(inside, lax.rem(place - first + stride * peers, stride) == 0)
            pl.when(owns)(owner_body)
            pl.when(jnp.logical_not(owns))(other_body)

    def drain(recv, sem, pieces):
        if pieces:
            ref = recv.at[pl.ds(0, pieces)]
            pltpu.make_async_copy(ref, ref, sem).wait()

    def drain_sends(cuts, place, peers, recv, rs_send, ag_send):
        owners = cuts[0] * cuts[1]

        def owner_body():
            drain(recv, rs_send, owners - 1)
            drain(recv, ag_send, peers - 1)

        either(cuts, place, peers, owner_body, lambda: drain(recv, rs_send, owners))

    p_cuts = split_tiles(count, band, width)
    q_cuts = split_columns(chips, half)
    p_owners, q_owners = p_cuts[0] * p_cuts[1], q_cuts[0] * q_cuts[1]
    members = cw // (half // q_cuts[1])
    own_group = index_of(q_cuts, chip) // members

    def split_factor(cols):
        high, low = halves(q_full[:, cols])
        return jnp.concatenate([high, low], axis=0)

    def tall_dot(left, factor):
        return lax.dot_general(left, factor, (((1,), (1,)), ((), ())), preferred_element_type=F32)

    block = max(256, width // p_cuts[1])
    blocks = width // block
    sharers = p_cuts[0] * (block // (width // p_cuts[1]))
    own_block = index_of(p_cuts, me) // sharers

    def block_of(index):
        return pl.ds(pl.multiple_of(index * block, block), block)

    def send_block(h, index):
        for j in range(sharers):
            place = index * sharers + j
            target = owner_of(p_cuts, place)

            @pl.when(target != me)
            def _():
                pltpu.make_async_remote_copy(
                    src_ref=p_part.at[window(p_cuts, width, place, h)],
                    dst_ref=p_recv.at[h, lax.rem(target - me + count, count) - 1],
                    send_sem=p_rs_send.at[h], recv_sem=p_rs_recv.at[h],
                    device_id=(target,), device_id_type=MESH,
                ).start()

    def band_factor(h, group):
        high, low = halves(q_full[rows_of(h), chunk(own_base, group)])
        return jnp.concatenate([high, low], axis=0)

    def absorb(h, group):
        factor = band_factor(h, group)
        cols = local(group)
        p_flat[h] += tall_dot(factor, m_hi[:, cols]) + tall_dot(factor, m_lo[:, cols])

    def absorb_last(h, group):
        factor = band_factor(h, group)
        cols = local(group)

        @pl.loop(0, blocks)
        def _(i):
            index = far_first(own_block, i + 1, blocks)
            rows = block_of(index)
            flat = p_flat[h, :, rows] + tall_dot(factor, m_hi[rows, cols]) + tall_dot(factor, m_lo[rows, cols])
            p_part[rows_of(h), rows] = flat[0:band] + flat[band:2 * band]
            send_block(h, index)

        p_flat[h] = jnp.zeros_like(p_flat[h])

    def merge(base, i, into):
        cols = chunk(base, i)
        product = jnp.dot(xt_v[...], dy_v[:, cols], preferred_element_type=F32)
        into[:, local(i)] = product + err_v[:, cols].astype(F32)

    def await_loads(base, i, slot):
        for load in chunk_loads(base, i, slot):
            load.wait()

    def first_factor(base, i):
        cols = chunk(base, i)
        factor = split_factor(cols)
        p_tall[...] += tall_dot(err_v[:, cols], factor)
        u_tall[...] += tall_dot(dy_v[:, cols], factor)

    def send_pair(i):
        pltpu.make_async_remote_copy(
            src_ref=rest.at[:, local(i)], dst_ref=pair.at[i],
            send_sem=pair_send, recv_sem=pair_recv.at[i],
            device_id=(partner,), device_id_type=MESH,
        ).start()

    p_tall[...] = jnp.zeros_like(p_tall)
    u_tall[...] = jnp.zeros_like(u_tall)
    pl.semaphore_wait(barrier, count - 1)
    start_load.wait()

    @pl.loop(0, groups)
    def _(i):
        await_loads(other_base, i, i)
        first_factor(other_base, i)

        @pl.when(i < EARLY)
        def _():
            merge(other_base, i, rest)
            send_pair(i)

    @pl.loop(0, groups)
    def _(i):
        await_loads(own_base, i, groups + i)
        first_factor(own_base, i)

    u_flat = u_tall[...].T
    high, low = halves(u_flat[0:rank] + u_flat[rank:2 * rank])
    u_split = jnp.concatenate([high, low], axis=0)

    @pl.loop(0, blocks)
    def _(i):
        index = far_first(own_block, i + 1, blocks)
        cols = block_of(index)
        flat = p_tall[cols, :].T + jnp.dot(u_split, x_v[:, cols], preferred_element_type=F32)
        p_part[:, cols] = flat[0:rank] + flat[rank:2 * rank]
        send_block(0, index)

    for h in range(1, STREAMS):

        @pl.loop(0, blocks)
        def _(i):
            send_block(h, far_first(own_block, i + 1, blocks))

    p_flat[...] = jnp.zeros_like(p_flat)

    @pl.loop(EARLY, groups)
    def _(i):
        merge(other_base, i, rest)
        pl.when(i < LATE)(lambda: send_pair(i))

    @pl.loop(0, groups // 2)
    def _(i):
        merge(own_base, i, merged)

    def add_pair():
        for i in range(LATE, groups):
            send_pair(i)

        @pl.loop(groups // 2, groups)
        def _(i):
            merge(own_base, i, merged)

        @pl.loop(0, groups)
        def _(i):
            pltpu.make_async_copy(pair.at[i], pair.at[i], pair_recv.at[i]).wait()
            high, low = halves(merged[:, local(i)] + pair[i])
            m_hi[:, local(i)] = high
            m_lo[:, local(i)] = low

        pltpu.make_async_copy(pair, pair, pair_send).wait()

    def orthogonalize(h):
        first = h * band
        if h == 0:
            lanes = lax.broadcasted_iota(jnp.int32, t_vecs.shape, 1)
            t_vecs[...] = (lanes == lax.broadcasted_iota(jnp.int32, t_vecs.shape, 0)).astype(F32)
        vecs[rows_of(h), :] = p_full[rows_of(h), :]

        def remove(unit, t_unit, rows):
            for below in rows:
                later = pl.ds(below, 8)
                coef = jnp.sum(p_full[later, :] * unit, axis=1, keepdims=True)
                vecs[later, :] = vecs[later, :] - coef * unit
                t_vecs[later, :] = t_vecs[later, :] - coef * t_unit

        for k in range(first):
            remove(basis[k:k + 1, :], t_mat[k:k + 1, :], range(first, first + band, 8))
        for base in range(first, first + band, 8):
            eight = pl.ds(base, 8)
            above, left, t_left = p_full[eight, :], vecs[eight, :], t_vecs[eight, :]
            done, t_done = [], []
            for k in range(8):
                row = left[k:k + 1, :]
                norm = jnp.sum(row * row, axis=1, keepdims=True) + 1.0
                coef = jnp.sum(above * row, axis=1, keepdims=True)
                inverse = lax.rsqrt(norm)
                unit = row * inverse
                t_unit = t_left[k:k + 1, :] * inverse
                done.append(unit)
                t_done.append(t_unit)
                if k < 7:
                    left = left - (coef * inverse) * unit
                    t_left = t_left - (coef * inverse) * t_unit
                remove(unit, t_unit, range(base + 8, first + band, 8))
            basis[eight, :] = jnp.concatenate(done, axis=0)
            t_mat[eight, :] = jnp.concatenate(t_done, axis=0)

    def sum_p(h):
        def body():
            mine = window(p_cuts, width, index_of(p_cuts, me), h)
            drain(p_recv.at[h], p_rs_recv.at[h], count - 1)
            p_full[mine] = p_part[mine] + jnp.sum(p_recv[h], axis=0)

            @pl.loop(1, count)
            def _(d):
                pltpu.make_async_remote_copy(
                    src_ref=p_full.at[mine], dst_ref=p_full.at[mine],
                    send_sem=p_ag_send.at[h], recv_sem=p_ag_recv.at[h],
                    device_id=(far_first(me, d, count),), device_id_type=MESH,
                ).start()

        either(p_cuts, me, count, body, lambda: None)

    def multiply(h):
        either(
            p_cuts, me, count,
            lambda: drain(p_recv.at[h], p_ag_recv.at[h], p_owners - 1),
            lambda: drain(p_recv.at[h], p_ag_recv.at[h], p_owners),
        )
        high, low = halves(p_full[rows_of(h), :])
        left = jnp.concatenate([high, low], axis=0)

        @pl.loop(0, groups)
        def _(i):
            group = far_first(own_group, i + 1, groups)
            cols = local(group)
            both = jnp.dot(left, m_hi[:, cols], preferred_element_type=F32)
            both += jnp.dot(left, m_lo[:, cols], preferred_element_type=F32)
            q_part[rows_of(h), cols] = both[0:band] + both[band:2 * band]

            for j in range(members):
                place = group * members + j
                target = owner_of(q_cuts, place)

                @pl.when(target != chip)
                def _():
                    pltpu.make_async_remote_copy(
                        src_ref=q_part.at[window(q_cuts, half, place, h)],
                        dst_ref=q_recv.at[h, lax.rem(target - chip + chips, chips) - 1],
                        send_sem=q_rs_send.at[h], recv_sem=q_rs_recv.at[h],
                        device_id=(2 * target + core,), device_id_type=MESH,
                    ).start()

    def sum_q(h):
        def body():
            drain(q_recv.at[h], q_rs_recv.at[h], chips - 1)
            index = index_of(q_cuts, chip)
            q_sum[rows_of(h), :] = q_part[window(q_cuts, half, index, h)] + jnp.sum(q_recv[h], axis=0)
            done = (h + 1) * band
            rotated = jnp.dot(
                t_mat[rows_of(h), 0:done], q_sum[0:done, :],
                precision=lax.Precision.HIGHEST, preferred_element_type=F32,
            )
            mine = window(q_cuts, half, index, h, own_base)
            q_full[mine] = rotated / count

            @pl.loop(1, chips)
            def _(d):
                pltpu.make_async_remote_copy(
                    src_ref=q_full.at[mine], dst_ref=q_full.at[mine],
                    send_sem=q_ag_send.at[h], recv_sem=q_ag_recv.at[h, own_group],
                    device_id=(2 * far_first(chip, d, chips) + core,), device_id_type=MESH,
                ).start()

        either(q_cuts, chip, chips, body, lambda: None)

    def await_group(h, group):
        def take(pieces):
            drain(q_recv.at[h], q_ag_recv.at[h, group], pieces)

        def own_or_other():
            pl.when(group == own_group)(lambda: take(members - 1))
            pl.when(group != own_group)(lambda: take(members))

        either(q_cuts, chip, chips, own_or_other, lambda: take(members))

    def drain_p(h):
        drain_sends(p_cuts, me, count, p_recv.at[h], p_rs_send.at[h], p_ag_send.at[h])

    def drain_q(h):
        drain_sends(q_cuts, chip, chips, q_recv.at[h], q_rs_send.at[h], q_ag_send.at[h])

    streams = range(STREAMS)

    @pl.loop(0, ITERS)
    def _(step):
        for h in streams:
            sum_p(h)
        pl.when(step == 0)(add_pair)
        for h in streams:
            multiply(h)
        for h in streams:
            orthogonalize(h)
            sum_q(h)
        for h in streams:
            drain_p(h)

        @pl.when(step < ITERS - 1)
        def _():
            for h in streams:
                @pl.loop(0, groups - 1)
                def _(i):
                    group = near_first(own_group, i, groups)
                    await_group(h, group)
                    absorb(h, group)

                group = near_first(own_group, groups - 1, groups)
                await_group(h, group)
                absorb_last(h, group)
            for h in streams:
                drain_q(h)

    tall = basis[...].T
    high, low = halves(tall)
    b_tall[:, 0:rank] = high
    b_tall[:, rank:2 * rank] = high
    b_tall[:, 2 * rank:3 * rank] = low

    def relay(base, group):
        cols = chunk(base, group)
        return pltpu.make_async_remote_copy(
            src_ref=q_full.at[:, cols], dst_ref=q_full.at[:, cols],
            send_sem=relay_send, recv_sem=relay_recv.at[group],
            device_id=(partner,), device_id_type=MESH,
        )

    @pl.loop(0, groups)
    def _(i):
        group = near_first(own_group, i, groups)
        for h in streams:
            await_group(h, group)
        relay(own_base, group).start()
        cols = local(group)
        err_own[:, cols] = (merged[:, cols] - recon(b_tall, q_full, chunk(own_base, group))).astype(BF16)

    @pl.loop(0, groups)
    def _(i):
        relay(other_base, i).wait_recv()

    for h in streams:
        drain_q(h)
    pltpu.make_async_copy(q_part, q_part, relay_send).wait()
    q_out[...] = q_full[...]


def recon(b_tall, q_full, cols):
    high, low = halves(q_full[:, cols])
    factor = jnp.concatenate([high, low, high], axis=0)
    return jnp.dot(b_tall[...], factor, preferred_element_type=F32)


def finish(
    err_own, rest, q_full, b_tall, master_hbm, err_out, q_out, master_out, tiles, master_v, load_sem, send_sem
):
    me = lax.axis_index(AXIS)
    core = lax.rem(me, 2)
    groups, _, cw = tiles.shape
    half = groups * cw
    own_base, other_base = core * half, (1 - core) * half
    load = pltpu.make_async_copy(master_hbm, master_v, load_sem)
    load.start()
    own_store = pltpu.make_async_copy(
        err_own, err_out.at[0, :, pl.ds(pl.multiple_of(own_base, half), half)], send_sem.at[groups]
    )
    own_store.start()
    q_store = pltpu.make_async_copy(q_full, q_out, send_sem.at[groups + 1])
    q_store.start()

    def store(i):
        cols = pl.ds(pl.multiple_of(other_base + i * cw, cw), cw)
        return pltpu.make_async_copy(tiles.at[i], err_out.at[0, :, cols], send_sem.at[i])

    @pl.loop(0, groups)
    def _(i):
        cols = pl.ds(pl.multiple_of(other_base + i * cw, cw), cw)
        local = pl.ds(pl.multiple_of(i * cw, cw), cw)
        tiles[i] = (rest[:, local] - recon(b_tall, q_full, cols)).astype(BF16)
        store(i).start()

    own = master_v.shape[1]
    span = max(own, 128)
    base = pl.multiple_of((me * own) // span * span, span)
    change = recon(b_tall, q_full, pl.ds(base, span))
    if own < span:
        change = pltpu.roll(change, lax.rem(span - lax.rem(me * own, span), span), 1)[:, 0:own]
    load.wait()
    master_v[...] = master_v[...] - 0.5 * change
    master_store = pltpu.make_async_copy(master_v, master_out, send_sem.at[groups + 2])
    master_store.start()

    @pl.loop(0, groups)
    def _(i):
        store(i).wait()

    own_store.wait()
    q_store.wait()
    master_store.wait()


def shards(inputs, out_grads, error_in, q_start, master):
    count = lax.axis_size(AXIS)
    tokens, width = inputs.shape
    ff = out_grads.shape[1]
    rank = q_start.shape[0]
    chips, half = count // 2, ff // 2
    groups = half // CHUNK
    hbm_spec = pl.BlockSpec(memory_space=pltpu.HBM)
    vmem_spec = pl.BlockSpec(memory_space=pltpu.VMEM)
    band = rank // STREAMS
    p_cuts, q_cuts = split_tiles(count, band, width), split_columns(chips, half)
    dma = pltpu.SemaphoreType.DMA
    parts = pl.pallas_call(
        functools.partial(kernel, count),
        out_shape=(
            pltpu.VMEM((width, half), BF16),
            pltpu.VMEM((width, half), F32),
            pltpu.VMEM((rank, ff), F32),
            pltpu.VMEM((width, 3 * rank), BF16),
        ),
        in_specs=[hbm_spec] * 4,
        out_specs=(vmem_spec,) * 4,
        scratch_shapes=[
            pltpu.VMEM((tokens, width), BF16),
            pltpu.VMEM((width, tokens), BF16),
            pltpu.VMEM((tokens, ff), BF16),
            pltpu.VMEM((width, ff), BF16),
            pltpu.VMEM((width, half), F32),
            pltpu.VMEM((groups, width, CHUNK), F32),
            pltpu.VMEM((width, half), BF16),
            pltpu.VMEM((width, half), BF16),
            pltpu.VMEM((rank, ff), F32),
            pltpu.VMEM((rank, half), F32),
            pltpu.VMEM((STREAMS, chips - 1, band, half // q_cuts[1]), F32),
            pltpu.VMEM((rank, half // q_cuts[1]), F32),
            pltpu.VMEM((rank, width), F32),
            pltpu.VMEM((rank, width), F32),
            pltpu.VMEM((STREAMS, count - 1, band // p_cuts[0], width // p_cuts[1]), F32),
            pltpu.VMEM((rank, width), F32),
            pltpu.VMEM((rank, width), F32),
            pltpu.VMEM((rank, 128), F32),
            pltpu.VMEM((rank, 128), F32),
            pltpu.VMEM((width, 2 * rank), F32),
            pltpu.VMEM((tokens, 2 * rank), F32),
            pltpu.VMEM((STREAMS, 2 * band, width), F32),
            dma, dma, dma((2 * groups,)), dma((2 * groups,)), dma, dma((groups,)), dma, dma((groups,)),
            dma((STREAMS,)), dma((STREAMS,)), dma((STREAMS,)), dma((STREAMS,)),
            dma((STREAMS,)), dma((STREAMS,)), dma((STREAMS,)), dma((STREAMS, groups)),
        ],
        compiler_params=pltpu.CompilerParams(
            collective_id=0, has_side_effects=True, vmem_limit_bytes=47 * 1024 * 1024
        ),
    )(inputs, out_grads, error_in, q_start)
    return pl.pallas_call(
        finish,
        out_shape=(
            jax.ShapeDtypeStruct(error_in.shape, BF16),
            jax.ShapeDtypeStruct(q_start.shape, F32),
            jax.ShapeDtypeStruct(master.shape, F32),
        ),
        in_specs=[vmem_spec] * 4 + [hbm_spec],
        out_specs=(hbm_spec,) * 3,
        scratch_shapes=[
            pltpu.VMEM((groups, width, CHUNK), BF16),
            pltpu.VMEM(master.shape, F32),
            dma, dma((groups + 3,)),
        ],
        compiler_params=pltpu.CompilerParams(vmem_limit_bytes=16 * 1024 * 1024),
    )(*parts, master)


def solution(mesh):
    return jax.shard_map(
        shards,
        mesh=mesh,
        in_specs=(P("rep", None), P("rep", None), P("rep", None, None), P(), P(None, "rep")),
        out_specs=(P("rep", None, None), P(), P(None, "rep")),
        check_vma=False,
    )
```

```python
import functools

import jax
import jax.numpy as jnp
from jax import lax
from jax.experimental import pallas as pl
from jax.experimental.pallas import tpu as pltpu
from jax.sharding import PartitionSpec as P

ITERS = 3
STREAMS = 2
MIDDLE = True
AXIS = "rep"
CHUNK = 512
EARLY, LATE = 2, 4
MESH = pl.DeviceIdType.MESH
F32, BF16 = jnp.float32, jnp.bfloat16


def split_tiles(count, rows, cols):
    pool, first = (count // 2, count // 4) if MIDDLE and count % 4 == 0 else (count, 0)
    col_cuts = min(pool, cols // 128)
    row_cuts = max(1, min(pool // col_cuts, rows // 8))
    return row_cuts, col_cuts, pool // (row_cuts * col_cuts), first


def split_columns(count, cols):
    col_cuts = min(count, cols // 128)
    return 1, col_cuts, count // col_cuts, 0


def halves(value):
    high = value.astype(BF16)
    return high, (value - high.astype(F32)).astype(BF16)


def far_part(own, step, parts):
    down = parts - 1 - step
    down = jnp.where(down <= own, down - 1, down)
    up = jnp.where(step >= own, step + 1, step)
    return jnp.where(step == parts - 1, own, jnp.where(2 * own < parts, down, up))


def near_part(own, step, parts):
    return far_part(own, parts - 1 - step, parts)


def far_first(own, step, count):
    size = count // 4
    if count % 4 or size & (size - 1):
        return lax.rem(own + step, count)
    plane = far_part(own // size, (step - 1) // size, 4)
    return plane * size + (lax.rem(own, size) ^ (size - 1 - lax.rem(step - 1, size)))


def kernel(
    count, x_hbm, dy_hbm, err_hbm, start_hbm,
    err_own, rest, q_out, b_tall,
    x_v, xt_v, dy_v, err_v, merged, pair, m_hi, m_lo,
    q_full, q_part, q_recv, q_sum, p_full, p_part, p_recv, vecs, basis, t_vecs, t_mat, p_tall, u_tall, p_flat,
    load_sem, start_sem, dy_sem, err_sem, pair_send, pair_recv, relay_send, relay_recv,
    p_rs_send, p_rs_recv, p_ag_send, p_ag_recv, q_rs_send, q_rs_recv, q_ag_send, q_ag_recv,
):
    me = lax.axis_index(AXIS)
    core, chip, chips = lax.rem(me, 2), me // 2, count // 2
    partner = me + 1 - 2 * core
    rank, width = p_full.shape
    band = rank // STREAMS
    ff = q_full.shape[1]
    half = ff // 2
    groups, _, cw = pair.shape
    own_base, other_base = core * half, (1 - core) * half

    def chunk(base, i):
        return pl.ds(pl.multiple_of(base + i * cw, cw), cw)

    def local(i):
        return pl.ds(pl.multiple_of(i * cw, cw), cw)

    def chunk_loads(base, i, slot):
        cols = chunk(base, i)
        return (
            pltpu.make_async_copy(dy_hbm.at[:, cols], dy_v.at[:, cols], dy_sem.at[slot]),
            pltpu.make_async_copy(err_hbm.at[0, :, cols], err_v.at[:, cols], err_sem.at[slot]),
        )

    def start_loads(base, i, slot):
        for load in chunk_loads(base, i, slot):
            load.start()

    pltpu.make_async_copy(x_hbm, x_v, load_sem).start()
    start_load = pltpu.make_async_copy(start_hbm, q_full, start_sem)
    start_load.start()
    start_loads(other_base, 0, 0)

    barrier = pltpu.get_barrier_semaphore()

    @pl.loop(1, count)
    def _(d):
        pl.semaphore_signal(barrier, inc=1, device_id=(lax.rem(me + d, count),), device_id_type=MESH)

    pltpu.make_async_copy(x_hbm, x_v, load_sem).wait()
    for i in range(1, groups):
        start_loads(other_base, i, i)
    for i in range(groups):
        start_loads(own_base, i, groups + i)
    xt_v[...] = x_v[...].T

    def rows_of(h):
        return pl.ds(h * band, band)

    def owner_of(cuts, index):
        return cuts[3] + index * cuts[2]

    def index_of(cuts, place):
        return jnp.clip((place - cuts[3]) // cuts[2], 0, cuts[0] * cuts[1] - 1)

    def window(cuts, cols, index, h, shift=0):
        row_cuts, col_cuts = cuts[:2]
        rows, cols = band // row_cuts, cols // col_cuts
        row = pl.multiple_of(h * band + lax.rem(index, row_cuts) * rows, rows)
        col = pl.multiple_of(shift + index // row_cuts * cols, cols)
        return pl.ds(row, rows), pl.ds(col, cols)

    def either(cuts, place, peers, owner_body, other_body):
        row_cuts, col_cuts, stride, first = cuts
        if row_cuts * col_cuts == peers:
            owner_body()
        else:
            inside = jnp.logical_and(place >= first, place < first + row_cuts * col_cuts * stride)
            owns = jnp.logical_and(inside, lax.rem(place - first + stride * peers, stride) == 0)
            pl.when(owns)(owner_body)
            pl.when(jnp.logical_not(owns))(other_body)

    def drain(recv, sem, pieces):
        if pieces:
            ref = recv.at[pl.ds(0, pieces)]
            pltpu.make_async_copy(ref, ref, sem).wait()

    def drain_sends(cuts, place, peers, recv, rs_send, ag_send):
        owners = cuts[0] * cuts[1]

        def owner_body():
            drain(recv, rs_send, owners - 1)
            drain(recv, ag_send, peers - 1)

        either(cuts, place, peers, owner_body, lambda: drain(recv, rs_send, owners))

    p_cuts = split_tiles(count, band, width)
    q_cuts = split_columns(chips, half)
    p_owners, q_owners = p_cuts[0] * p_cuts[1], q_cuts[0] * q_cuts[1]
    members = cw // (half // q_cuts[1])
    own_group = index_of(q_cuts, chip) // members

    def split_factor(cols):
        high, low = halves(q_full[:, cols])
        return jnp.concatenate([high, low], axis=0)

    def tall_dot(left, factor):
        return lax.dot_general(left, factor, (((1,), (1,)), ((), ())), preferred_element_type=F32)

    block = max(256, width // p_cuts[1])
    blocks = width // block
    sharers = p_cuts[0] * (block // (width // p_cuts[1]))
    own_block = index_of(p_cuts, me) // sharers

    def block_of(index):
        return pl.ds(pl.multiple_of(index * block, block), block)

    def send_block(h, index):
        for j in range(sharers):
            place = index * sharers + j
            target = owner_of(p_cuts, place)

            @pl.when(target != me)
            def _():
                pltpu.make_async_remote_copy(
                    src_ref=p_part.at[window(p_cuts, width, place, h)],
                    dst_ref=p_recv.at[h, lax.rem(target - me + count, count) - 1],
                    send_sem=p_rs_send.at[h], recv_sem=p_rs_recv.at[h],
                    device_id=(target,), device_id_type=MESH,
                ).start()

    def band_factor(h, group):
        high, low = halves(q_full[rows_of(h), chunk(own_base, group)])
        return jnp.concatenate([high, low], axis=0)

    def turn():
        @pl.loop(0, groups)
        def _(i):
            slot = pl.ds(pl.multiple_of(i * width, width), width)
            err_v[0:cw, slot] = m_hi[:, local(i)].T
            err_v[cw:2 * cw, slot] = m_lo[:, local(i)].T

    def across(factor, group, shift, size):
        slot = pl.ds(pl.multiple_of(group * width + shift, size), size)
        return jnp.dot(factor, err_v[0:cw, slot], preferred_element_type=F32) + jnp.dot(
            factor, err_v[cw:2 * cw, slot], preferred_element_type=F32
        )

    def absorb(h, group):
        p_flat[h] += across(band_factor(h, group), group, 0, width)

    def absorb_last(h, group):
        factor = band_factor(h, group)

        @pl.loop(0, blocks)
        def _(i):
            index = far_part(own_block, i, blocks)
            rows = block_of(index)
            flat = p_flat[h, :, rows] + across(factor, group, index * block, block)
            p_part[rows_of(h), rows] = flat[0:band] + flat[band:2 * band]
            send_block(h, index)

        p_flat[h] = jnp.zeros_like(p_flat[h])

    def merge(base, i, into):
        cols = chunk(base, i)
        product = jnp.dot(xt_v[...], dy_v[:, cols], preferred_element_type=F32)
        into[:, local(i)] = product + err_v[:, cols].astype(F32)

    def await_loads(base, i, slot):
        for load in chunk_loads(base, i, slot):
            load.wait()

    def first_factor(base, i):
        cols = chunk(base, i)
        factor = split_factor(cols)
        p_tall[...] += tall_dot(err_v[:, cols], factor)
        u_tall[...] += tall_dot(dy_v[:, cols], factor)

    def send_pair(i):
        pltpu.make_async_remote_copy(
            src_ref=rest.at[:, local(i)], dst_ref=pair.at[i],
            send_sem=pair_send, recv_sem=pair_recv.at[i],
            device_id=(partner,), device_id_type=MESH,
        ).start()

    p_tall[...] = jnp.zeros_like(p_tall)
    u_tall[...] = jnp.zeros_like(u_tall)
    pl.semaphore_wait(barrier, count - 1)
    start_load.wait()

    @pl.loop(0, groups)
    def _(i):
        await_loads(other_base, i, i)
        first_factor(other_base, i)

        @pl.when(i < EARLY)
        def _():
            merge(other_base, i, rest)
            send_pair(i)

    @pl.loop(0, groups)
    def _(i):
        await_loads(own_base, i, groups + i)
        first_factor(own_base, i)

    u_flat = u_tall[...].T
    high, low = halves(u_flat[0:rank] + u_flat[rank:2 * rank])
    u_split = jnp.concatenate([high, low], axis=0)

    @pl.loop(0, blocks)
    def _(i):
        index = far_part(own_block, i, blocks)
        cols = block_of(index)
        flat = p_tall[cols, :].T + jnp.dot(u_split, x_v[:, cols], preferred_element_type=F32)
        p_part[:, cols] = flat[0:rank] + flat[rank:2 * rank]
        send_block(0, index)

    for h in range(1, STREAMS):

        @pl.loop(0, blocks)
        def _(i):
            send_block(h, far_part(own_block, i, blocks))

    p_flat[...] = jnp.zeros_like(p_flat)

    @pl.loop(EARLY, groups)
    def _(i):
        merge(other_base, i, rest)
        pl.when(i < LATE)(lambda: send_pair(i))

    @pl.loop(0, groups // 2)
    def _(i):
        merge(own_base, i, merged)

    def add_pair():
        for i in range(LATE, groups):
            send_pair(i)

        @pl.loop(groups // 2, groups)
        def _(i):
            merge(own_base, i, merged)

        @pl.loop(0, groups)
        def _(i):
            pltpu.make_async_copy(pair.at[i], pair.at[i], pair_recv.at[i]).wait()
            high, low = halves(merged[:, local(i)] + pair[i])
            m_hi[:, local(i)] = high
            m_lo[:, local(i)] = low

        pltpu.make_async_copy(pair, pair, pair_send).wait()

    def orthogonalize(h):
        first = h * band
        if h == 0:
            lanes = lax.broadcasted_iota(jnp.int32, t_vecs.shape, 1)
            t_vecs[...] = (lanes == lax.broadcasted_iota(jnp.int32, t_vecs.shape, 0)).astype(F32)
        vecs[rows_of(h), :] = p_full[rows_of(h), :]

        def remove(unit, t_unit, rows):
            for below in rows:
                later = pl.ds(below, 8)
                coef = jnp.sum(p_full[later, :] * unit, axis=1, keepdims=True)
                vecs[later, :] = vecs[later, :] - coef * unit
                t_vecs[later, :] = t_vecs[later, :] - coef * t_unit

        for k in range(first):
            remove(basis[k:k + 1, :], t_mat[k:k + 1, :], range(first, first + band, 8))
        for base in range(first, first + band, 8):
            eight = pl.ds(base, 8)
            above, left, t_left = p_full[eight, :], vecs[eight, :], t_vecs[eight, :]
            done, t_done = [], []
            for k in range(8):
                row = left[k:k + 1, :]
                norm = jnp.sum(row * row, axis=1, keepdims=True) + 1.0
                coef = jnp.sum(above * row, axis=1, keepdims=True)
                inverse = lax.rsqrt(norm)
                unit = row * inverse
                t_unit = t_left[k:k + 1, :] * inverse
                done.append(unit)
                t_done.append(t_unit)
                if k < 7:
                    left = left - (coef * inverse) * unit
                    t_left = t_left - (coef * inverse) * t_unit
                remove(unit, t_unit, range(base + 8, first + band, 8))
            basis[eight, :] = jnp.concatenate(done, axis=0)
            t_mat[eight, :] = jnp.concatenate(t_done, axis=0)

    def sum_p(h):
        def body():
            mine = window(p_cuts, width, index_of(p_cuts, me), h)
            drain(p_recv.at[h], p_rs_recv.at[h], count - 1)
            p_full[mine] = p_part[mine] + jnp.sum(p_recv[h], axis=0)

            @pl.loop(1, count)
            def _(d):
                pltpu.make_async_remote_copy(
                    src_ref=p_full.at[mine], dst_ref=p_full.at[mine],
                    send_sem=p_ag_send.at[h], recv_sem=p_ag_recv.at[h],
                    device_id=(far_first(me, d, count),), device_id_type=MESH,
                ).start()

        either(p_cuts, me, count, body, lambda: None)

    def multiply(h):
        either(
            p_cuts, me, count,
            lambda: drain(p_recv.at[h], p_ag_recv.at[h], p_owners - 1),
            lambda: drain(p_recv.at[h], p_ag_recv.at[h], p_owners),
        )
        high, low = halves(p_full[rows_of(h), :])
        left = jnp.concatenate([high, low], axis=0)

        @pl.loop(0, groups)
        def _(i):
            group = far_part(own_group, i, groups)
            cols = local(group)
            both = jnp.dot(left, m_hi[:, cols], preferred_element_type=F32)
            both += jnp.dot(left, m_lo[:, cols], preferred_element_type=F32)
            q_part[rows_of(h), cols] = both[0:band] + both[band:2 * band]

            for j in range(members):
                place = group * members + j
                target = owner_of(q_cuts, place)

                @pl.when(target != chip)
                def _():
                    pltpu.make_async_remote_copy(
                        src_ref=q_part.at[window(q_cuts, half, place, h)],
                        dst_ref=q_recv.at[h, lax.rem(target - chip + chips, chips) - 1],
                        send_sem=q_rs_send.at[h], recv_sem=q_rs_recv.at[h],
                        device_id=(2 * target + core,), device_id_type=MESH,
                    ).start()

    def sum_q(h):
        def body():
            drain(q_recv.at[h], q_rs_recv.at[h], chips - 1)
            index = index_of(q_cuts, chip)
            q_sum[rows_of(h), :] = q_part[window(q_cuts, half, index, h)] + jnp.sum(q_recv[h], axis=0)
            done = (h + 1) * band
            rotated = jnp.dot(
                t_mat[rows_of(h), 0:done], q_sum[0:done, :],
                precision=lax.Precision.HIGHEST, preferred_element_type=F32,
            )
            mine = window(q_cuts, half, index, h, own_base)
            q_full[mine] = rotated / count

            @pl.loop(1, chips)
            def _(d):
                pltpu.make_async_remote_copy(
                    src_ref=q_full.at[mine], dst_ref=q_full.at[mine],
                    send_sem=q_ag_send.at[h], recv_sem=q_ag_recv.at[h, own_group],
                    device_id=(2 * far_first(chip, d, chips) + core,), device_id_type=MESH,
                ).start()

        either(q_cuts, chip, chips, body, lambda: None)

    def await_group(h, group):
        def take(pieces):
            drain(q_recv.at[h], q_ag_recv.at[h, group], pieces)

        def own_or_other():
            pl.when(group == own_group)(lambda: take(members - 1))
            pl.when(group != own_group)(lambda: take(members))

        either(q_cuts, chip, chips, own_or_other, lambda: take(members))

    def drain_p(h):
        drain_sends(p_cuts, me, count, p_recv.at[h], p_rs_send.at[h], p_ag_send.at[h])

    def drain_q(h):
        drain_sends(q_cuts, chip, chips, q_recv.at[h], q_rs_send.at[h], q_ag_send.at[h])

    streams = range(STREAMS)

    @pl.loop(0, ITERS)
    def _(step):
        for h in streams:
            sum_p(h)
        pl.when(step == 0)(add_pair)
        for h in streams:
            multiply(h)
        for h in streams:
            orthogonalize(h)
            sum_q(h)
        pl.when(step == 0)(turn)
        for h in streams:
            drain_p(h)

        @pl.when(step < ITERS - 1)
        def _():
            for h in streams:
                @pl.loop(0, groups - 1)
                def _(i):
                    group = near_part(own_group, i, groups)
                    await_group(h, group)
                    absorb(h, group)

                group = near_part(own_group, groups - 1, groups)
                await_group(h, group)
                absorb_last(h, group)
            for h in streams:
                drain_q(h)

    tall = basis[...].T
    high, low = halves(tall)
    b_tall[:, 0:rank] = high
    b_tall[:, rank:2 * rank] = high
    b_tall[:, 2 * rank:3 * rank] = low

    def relay(base, group):
        cols = chunk(base, group)
        return pltpu.make_async_remote_copy(
            src_ref=q_full.at[:, cols], dst_ref=q_full.at[:, cols],
            send_sem=relay_send, recv_sem=relay_recv.at[group],
            device_id=(partner,), device_id_type=MESH,
        )

    @pl.loop(0, groups)
    def _(i):
        group = near_part(own_group, i, groups)
        for h in streams:
            await_group(h, group)
        relay(own_base, group).start()
        cols = local(group)
        err_own[:, cols] = (merged[:, cols] - recon(b_tall, q_full, chunk(own_base, group))).astype(BF16)

    @pl.loop(0, groups)
    def _(i):
        relay(other_base, i).wait_recv()

    for h in streams:
        drain_q(h)
    pltpu.make_async_copy(q_part, q_part, relay_send).wait()
    q_out[...] = q_full[...]


def recon(b_tall, q_full, cols):
    high, low = halves(q_full[:, cols])
    factor = jnp.concatenate([high, low, high], axis=0)
    return jnp.dot(b_tall[...], factor, preferred_element_type=F32)


def finish(
    err_own, rest, q_full, b_tall, master_hbm, err_out, q_out, master_out, tiles, master_v, load_sem, send_sem
):
    me = lax.axis_index(AXIS)
    core = lax.rem(me, 2)
    groups, _, cw = tiles.shape
    half = groups * cw
    own_base, other_base = core * half, (1 - core) * half
    load = pltpu.make_async_copy(master_hbm, master_v, load_sem)
    load.start()
    own_store = pltpu.make_async_copy(
        err_own, err_out.at[0, :, pl.ds(pl.multiple_of(own_base, half), half)], send_sem.at[groups]
    )
    own_store.start()
    q_store = pltpu.make_async_copy(q_full, q_out, send_sem.at[groups + 1])
    q_store.start()

    def store(i):
        cols = pl.ds(pl.multiple_of(other_base + i * cw, cw), cw)
        return pltpu.make_async_copy(tiles.at[i], err_out.at[0, :, cols], send_sem.at[i])

    @pl.loop(0, groups)
    def _(i):
        cols = pl.ds(pl.multiple_of(other_base + i * cw, cw), cw)
        local = pl.ds(pl.multiple_of(i * cw, cw), cw)
        tiles[i] = (rest[:, local] - recon(b_tall, q_full, cols)).astype(BF16)
        store(i).start()

    own = master_v.shape[1]
    span = max(own, 128)
    base = pl.multiple_of((me * own) // span * span, span)
    change = recon(b_tall, q_full, pl.ds(base, span))
    if own < span:
        change = pltpu.roll(change, lax.rem(span - lax.rem(me * own, span), span), 1)[:, 0:own]
    load.wait()
    master_v[...] = master_v[...] - 0.5 * change
    master_store = pltpu.make_async_copy(master_v, master_out, send_sem.at[groups + 2])
    master_store.start()

    @pl.loop(0, groups)
    def _(i):
        store(i).wait()

    own_store.wait()
    q_store.wait()
    master_store.wait()


def shards(inputs, out_grads, error_in, q_start, master):
    count = lax.axis_size(AXIS)
    tokens, width = inputs.shape
    ff = out_grads.shape[1]
    rank = q_start.shape[0]
    chips, half = count // 2, ff // 2
    groups = half // CHUNK
    assert 2 * CHUNK <= width and groups * width <= ff
    hbm_spec = pl.BlockSpec(memory_space=pltpu.HBM)
    vmem_spec = pl.BlockSpec(memory_space=pltpu.VMEM)
    band = rank // STREAMS
    p_cuts, q_cuts = split_tiles(count, band, width), split_columns(chips, half)
    dma = pltpu.SemaphoreType.DMA
    parts = pl.pallas_call(
        functools.partial(kernel, count),
        out_shape=(
            pltpu.VMEM((width, half), BF16),
            pltpu.VMEM((width, half), F32),
            pltpu.VMEM((rank, ff), F32),
            pltpu.VMEM((width, 3 * rank), BF16),
        ),
        in_specs=[hbm_spec] * 4,
        out_specs=(vmem_spec,) * 4,
        scratch_shapes=[
            pltpu.VMEM((tokens, width), BF16),
            pltpu.VMEM((width, tokens), BF16),
            pltpu.VMEM((tokens, ff), BF16),
            pltpu.VMEM((width, ff), BF16),
            pltpu.VMEM((width, half), F32),
            pltpu.VMEM((groups, width, CHUNK), F32),
            pltpu.VMEM((width, half), BF16),
            pltpu.VMEM((width, half), BF16),
            pltpu.VMEM((rank, ff), F32),
            pltpu.VMEM((rank, half), F32),
            pltpu.VMEM((STREAMS, chips - 1, band, half // q_cuts[1]), F32),
            pltpu.VMEM((rank, half // q_cuts[1]), F32),
            pltpu.VMEM((rank, width), F32),
            pltpu.VMEM((rank, width), F32),
            pltpu.VMEM((STREAMS, count - 1, band // p_cuts[0], width // p_cuts[1]), F32),
            pltpu.VMEM((rank, width), F32),
            pltpu.VMEM((rank, width), F32),
            pltpu.VMEM((rank, 128), F32),
            pltpu.VMEM((rank, 128), F32),
            pltpu.VMEM((width, 2 * rank), F32),
            pltpu.VMEM((tokens, 2 * rank), F32),
            pltpu.VMEM((STREAMS, 2 * band, width), F32),
            dma, dma, dma((2 * groups,)), dma((2 * groups,)), dma, dma((groups,)), dma, dma((groups,)),
            dma((STREAMS,)), dma((STREAMS,)), dma((STREAMS,)), dma((STREAMS,)),
            dma((STREAMS,)), dma((STREAMS,)), dma((STREAMS,)), dma((STREAMS, groups)),
        ],
        compiler_params=pltpu.CompilerParams(
            collective_id=0, has_side_effects=True, vmem_limit_bytes=47 * 1024 * 1024
        ),
    )(inputs, out_grads, error_in, q_start)
    return pl.pallas_call(
        finish,
        out_shape=(
            jax.ShapeDtypeStruct(error_in.shape, BF16),
            jax.ShapeDtypeStruct(q_start.shape, F32),
            jax.ShapeDtypeStruct(master.shape, F32),
        ),
        in_specs=[vmem_spec] * 4 + [hbm_spec],
        out_specs=(hbm_spec,) * 3,
        scratch_shapes=[
            pltpu.VMEM((groups, width, CHUNK), BF16),
            pltpu.VMEM(master.shape, F32),
            dma, dma((groups + 3,)),
        ],
        compiler_params=pltpu.CompilerParams(vmem_limit_bytes=16 * 1024 * 1024),
    )(*parts, master)


def solution(mesh):
    return jax.shard_map(
        shards,
        mesh=mesh,
        in_specs=(P("rep", None), P("rep", None), P("rep", None, None), P(), P(None, "rep")),
        out_specs=(P("rep", None, None), P(), P(None, "rep")),
        check_vma=False,
    )
```
